32 devices in a mesh: grp: 4 (over y, x), vir: 8 (over z, core).
Axes of the slice: x: 2, y: 2, z: 4, core: 2. Of those that a mesh axis runs over, the one named last changes fastest.
Arguments:
- triplets: int32 [24, 3], P('grp'), may hold values from 0 to 4, as said below
- counts: int32 [4], P('grp'), may hold values from 1 to 6, as said below
- weights: int32 [24], P('grp'), may hold values from 1 to 3
- a_pick: int32 [16], P('vir'), may hold values from 0 to 895, as said below
- occ_energy: float32 [5], replicated, may hold values from -2 to -0.5
- vir_energy: float32 [896], replicated, may hold values from 0.3 to 3
- ints_vvvo: bfloat16 [5, 16, 896, 896], P(None, 'vir'), may hold values from -0.1875 to 0.1875
- t2pair: bfloat16 [5, 5, 896, 896], P(None, None, 'vir'), may hold values from -6 to 6
- t2hole: bfloat16 [5, 60, 16, 896], P(None, None, 'vir'), may hold values from -6 to 6
- ints_hole: bfloat16 [5, 5, 60, 896], replicated, may hold values from -0.75 to 0.75
Outputs:
- trip_energy: float32 [24], P('grp')
- orbital_energy: float32 [16], P('vir')
The draws below stay inside these ranges and needn't reach their ends.
Inputs may be any that keep to these rules, and one draw needn't show every extreme that they name: `triplets`: each row holds occupied indices i <= j <= k. `counts`: some group has all 6 slots live. `a_pick`: the entries are distinct.
All inputs are finite; a program needn't handle non-finite values.
Results may differ from the reference program's by a relative error of at most 0.0003.
Values may be sent and summed in bfloat16 or wider, within the bound.
A program may use at most 64 MiB of HBM per device.

```python
import math
import jax
import jax.numpy as jnp
from jax import lax

V = 896
O = 60
OW = 5
NT = 6
GROUPS = 4
TRIPLETS = 24
AW = 16


def draw_triplets(key, part):
    values = jax.random.randint(key, (TRIPLETS, 3), 0, OW)
    return jnp.sort(values, axis=1).astype(jnp.int32)


def draw_counts(key, part):
    filled = jax.random.randint(jax.random.fold_in(key, 11), (GROUPS,), 1, NT + 1)
    chosen = jax.random.randint(jax.random.fold_in(key, 12), (), 0, GROUPS)
    groups_iota = jnp.arange(GROUPS, dtype=jnp.int32)
    return jnp.where(groups_iota == chosen, NT, filled).astype(jnp.int32)


def draw_a_pick(key, part):
    order = jax.random.permutation(jax.random.fold_in(key, 21), V)
    return order[:AW].astype(jnp.int32)


def with_ends(array, stream_key, least, top_value):
    extent = array.shape
    place = [jax.random.randint(jax.random.fold_in(stream_key, axis), (), 0, extent[axis]) for axis in range(len(extent))]
    array = array.at[tuple(place)].set(least)
    longest = extent.index(max(extent))
    place[longest] = (place[longest] + 1) % extent[longest]
    return array.at[tuple(place)].set(top_value)


def block_scale(own_key, extent, cuts, least, largest):
    level = 1.0
    for dim, parts in cuts:
        heights = jax.random.uniform(jax.random.fold_in(jax.random.fold_in(own_key, 6), dim), (parts,), jnp.float32, least / len(cuts), largest / len(cuts))
        level = level * jnp.repeat(jnp.exp(heights), extent[dim] // parts).reshape((-1,) + (1,) * (len(extent) - 1 - dim))
    return level


def scatter_about(key, shape, scale, reach, pieces=(), kind=jnp.bfloat16):
    values = scale * jax.random.normal(key, shape, jnp.float32)
    if pieces:
        values = values * block_scale(key, shape, pieces, -0.22, 0.18)
    return jnp.clip(values, -reach, reach).astype(kind)


def setup_inputs(seed: int = 0) -> dict:
    key_of = jax.random.split(jax.random.key(seed), 11)
    triplets = draw_triplets(jax.random.fold_in(key_of[10], 71), 0)
    counts = draw_counts(jax.random.fold_in(key_of[10], 71), 0)
    weights = with_ends(jax.random.randint(key_of[2], (TRIPLETS,), 1, 4), jax.random.fold_in(key_of[2], 1), 1, 3).astype(jnp.int32)
    a_pick = draw_a_pick(jax.random.fold_in(key_of[10], 71), 0)
    occ_energy = jnp.clip(jax.random.uniform(key_of[4], (OW,), jnp.float32, -2.0, -0.5), -2.0, -0.5)
    vir_energy = jnp.clip(jnp.exp(jax.random.uniform(key_of[5], (V,), jnp.float32, math.log(0.3), math.log(3.0))), 0.3, 3.0)
    ints_vvvo = scatter_about(key_of[6], (OW, AW, V, V), V ** -0.5, 0.1875, ((1, 8),))
    t2pair = scatter_about(key_of[7], (OW, OW, V, V), 1.0, 6.0, ((2, 8),))
    t2hole = scatter_about(key_of[8], (OW, O, AW, V), 1.0, 6.0, ((2, 8),))
    ints_hole = scatter_about(key_of[9], (OW, OW, O, V), O ** -0.5, 0.75)
    return dict(triplets=triplets, counts=counts, weights=weights, a_pick=a_pick, occ_energy=occ_energy, vir_energy=vir_energy, ints_vvvo=ints_vvvo, t2pair=t2pair, t2hole=t2hole, ints_hole=ints_hole)


def reference(triplets, counts, weights, a_pick, occ_energy, vir_energy, ints_vvvo, t2pair, t2hole, ints_hole):
    a_energy = vir_energy[a_pick]
    width = vir_energy.shape[0]
    window = a_pick.shape[0]

    def one_slot(orbital, slot_index):
        trip_row = triplets[slot_index]
        occ_i = trip_row[0]
        occ_j = trip_row[1]
        occ_k = trip_row[2]
        integral_slab = ints_vvvo[occ_k].astype(jnp.float32)
        pair_slab = t2pair[occ_j, occ_k].astype(jnp.float32)
        hole_amps = t2hole[occ_i].astype(jnp.float32)
        hole_ints = ints_hole[occ_k, occ_j].astype(jnp.float32)
        particle = jnp.einsum('abd,cd->abc', integral_slab, pair_slab, precision=lax.Precision.HIGHEST)
        holes_term = jnp.einsum('lab,lc->abc', hole_amps, hole_ints, precision=lax.Precision.HIGHEST)
        amplitude = particle - holes_term
        occ_shift = occ_energy[occ_i] + occ_energy[occ_j] + occ_energy[occ_k]
        denominator = a_energy[:, None, None] + vir_energy[None, :, None] + vir_energy[None, None, :] - occ_shift
        live = (slot_index % NT) < counts[slot_index // NT]
        factor = jnp.where(live, -weights[slot_index].astype(jnp.float32) / (width * width), jnp.float32(0.0))
        energy = factor * jnp.sum(amplitude * amplitude / denominator, axis=(1, 2))
        return orbital + energy, jnp.sum(energy) / window

    orbital, trip_energy = lax.scan(one_slot, jnp.zeros((window,), jnp.float32), jnp.arange(TRIPLETS, dtype=jnp.int32))
    return trip_energy, orbital
```

```python
import functools

import jax
import jax.numpy as jnp
from jax import lax
from jax.experimental import pallas as pl
from jax.experimental.pallas import tpu as pltpu
from jax.sharding import PartitionSpec as P

LANES = 128
VMEM_LIMIT = 60 * 1024 * 1024


def cdiv(a, b):
    return (a + b - 1) // b


class Plan:
    def __init__(self, groups, nvir, slots, ow, width):
        self.groups, self.nvir, self.slots, self.ow, self.width = groups, nvir, slots, ow, width
        self.total = groups * slots
        self.tiles = width // LANES
        self.rows = LANES // nvir
        self.pairs = min(ow * (ow + 1) // 2, self.total)
        self.units = cdiv(self.tiles * self.pairs, groups)
        self.keys = ow * ow
        self.n_pairs = 0
        self.n_units = 1
        self.first = 2
        self.key = self.first + self.pairs + 1
        self.order = self.key + self.pairs + 1
        self.occ_i = self.order + self.total
        self.unit_pair = self.occ_i + self.total
        self.unit_tile = self.unit_pair + self.units
        self.size = self.unit_tile + self.units

    def aligned(self):
        return self.rows % 16 == 0 and self.nvir % 2 == 0


def plan_kernel(plan, with_rows, meta, *refs):
    if with_rows:
        t2pair, table, send, count, place, sems = refs
    else:
        table, count, place = refs
    group = lax.axis_index("grp")
    slots, ow = plan.slots, plan.ow

    def fields(n):
        g = n // slots
        s = n % slots
        live = s < meta[g, 0]
        at = 1 + 3 * s
        return live, meta[g, at], meta[g, at + 1], meta[g, at + 2]

    for key in range(plan.keys):
        count[key] = 0
    for n in range(plan.total):
        live, i, j, k = fields(n)
        key = k * ow + j
        count[key] = count[key] + live.astype(jnp.int32)
    pair = jnp.int32(0)
    pos = jnp.int32(0)
    table[plan.key] = 0
    for key in range(plan.keys):
        here = count[key]
        place[key] = pos

        @pl.when(here > 0)
        def _():
            table[plan.first + pair] = pos
            table[plan.key + pair] = key

        pair = pair + (here > 0).astype(jnp.int32)
        pos = pos + here
    table[plan.first + pair] = pos
    n_units = (plan.tiles * pair + plan.groups - 1) // plan.groups
    table[plan.n_pairs] = pair
    table[plan.n_units] = n_units
    for n in range(plan.total):
        live, i, j, k = fields(n)
        key = k * ow + j

        @pl.when(live)
        def _():
            at = place[key]
            table[plan.order + at] = n
            table[plan.occ_i + at] = i
            place[key] = at + 1

    for u in range(plan.units):
        q = u * plan.groups + group
        p = q // plan.tiles
        real = p < pair
        table[plan.unit_pair + u] = jnp.where(real, p, plan.pairs)
        table[plan.unit_tile + u] = q % plan.tiles
        if with_rows:
            key = table[plan.key + jnp.where(real, p, 0)]
            tile = pl.multiple_of((q % plan.tiles) * plan.rows, plan.rows)
            pltpu.make_async_copy(
                t2pair.at[key % ow, key // ow, pl.ds(tile, plan.rows), :], send.at[u], sems.at[u]
            ).start()
    if with_rows:
        for u in range(plan.units):
            pltpu.make_async_copy(t2pair.at[0, 0, pl.ds(0, plan.rows), :], send.at[u], sems.at[u]).wait()


def make_plan(plan, meta, t2pair):
    with_rows = plan.aligned()
    smem = pl.BlockSpec(memory_space=pltpu.SMEM)
    table_shape = jax.ShapeDtypeStruct((plan.size,), jnp.int32)
    scratch = [pltpu.SMEM((plan.keys,), jnp.int32), pltpu.SMEM((plan.keys,), jnp.int32)]
    if with_rows:
        send_shape = jax.ShapeDtypeStruct((plan.units, plan.rows, plan.width), t2pair.dtype)
        return pl.pallas_call(
            functools.partial(plan_kernel, plan, True),
            out_shape=(table_shape, send_shape),
            in_specs=[smem, pl.BlockSpec(memory_space=pl.ANY)],
            out_specs=(smem, pl.BlockSpec(memory_space=pltpu.VMEM)),
            scratch_shapes=scratch + [pltpu.SemaphoreType.DMA((plan.units,))],
            name="plan",
        )(meta, t2pair)
    table = pl.pallas_call(
        functools.partial(plan_kernel, plan, False),
        out_shape=table_shape,
        in_specs=[smem],
        out_specs=smem,
        scratch_shapes=scratch,
        name="plan",
    )(meta)
    unit_pair = lax.dynamic_slice_in_dim(table, plan.unit_pair, plan.units)
    tile = lax.dynamic_slice_in_dim(table, plan.unit_tile, plan.units)
    key = table[plan.key + jnp.where(unit_pair < table[0], unit_pair, 0)]
    cut = t2pair.reshape(plan.ow, plan.ow, plan.tiles, plan.rows, plan.width)
    return table, cut[key % plan.ow, key // plan.ow, tile]


def move_kernel(plan, batches, send, gath, ssem, rsem, lsem):
    me = lax.axis_index("vir")
    chips = plan.nvir // 2
    z = me // 2
    core = me % 2
    partner = me + 1 - 2 * core
    right = jnp.minimum(z + 1, chips - 1) * 2 + core
    left = jnp.maximum(z - 1, 0) * 2 + core
    has_right = z < chips - 1
    has_left = z > 0
    barrier = pltpu.get_barrier_semaphore()
    pl.semaphore_signal(barrier, inc=1, device_id={"vir": partner})

    @pl.when(has_right)
    def _():
        pl.semaphore_signal(barrier, inc=1, device_id={"vir": right})

    @pl.when(has_left)
    def _():
        pl.semaphore_signal(barrier, inc=1, device_id={"vir": left})

    pl.semaphore_wait(barrier, 1 + has_right.astype(jnp.int32) + has_left.astype(jnp.int32))

    def copy(b, v, to, way, own=False):
        lo, n = batches[b]
        block = gath.at[v, pl.ds(lo, n)]
        return pltpu.make_async_remote_copy(
            src_ref=send.at[pl.ds(lo, n)] if own else block,
            dst_ref=block,
            send_sem=ssem.at[way, v, b],
            recv_sem=rsem.at[v, b],
            device_id={"vir": to},
        )

    def local(b):
        lo, n = batches[b]
        return pltpu.make_async_copy(send.at[pl.ds(lo, n)], gath.at[me, pl.ds(lo, n)], lsem.at[b])

    steps = range(len(batches))

    def every(act):
        for b in steps:
            act(has_right, b, me, right, 0, True, False)
            act(has_left, b, me, left, 1, True, False)
            act(None, b, me, partner, 2, True, False)
        for d in range(1, chips):
            for b in steps:
                for way, source, there, more, to in (
                    (0, me - 2 * d, z - d >= 0, has_right, right),
                    (1, me + 2 * d, z + d < chips, has_left, left),
                ):
                    act(there, b, source, partner, 2, False, True)
                    act(jnp.logical_and(there, more), b, source, to, way, False, False)

    def start(cond, b, source, to, way, own, arrives):
        def go():
            one = copy(b, source, to, way, own)
            if arrives:
                one.wait_recv()
            one.start()

        if cond is None:
            go()
        else:
            pl.when(cond)(go)

    def finish(cond, b, source, to, way, own, arrives):
        def go():
            copy(b, source, to, way, own).wait_send()

        if cond is None:
            go()
        else:
            pl.when(cond)(go)

    for b in steps:
        local(b).start()
    every(start)
    for other in range(chips):
        for b in steps:
            copy(b, 2 * other + 1 - core, partner, 2).wait_recv()
    every(finish)
    for b in steps:
        local(b).wait()


def move(plan, send, units, batch, number):
    batches = [(lo, min(batch, units - lo)) for lo in range(0, units, batch)]
    count = len(batches)
    return pl.pallas_call(
        functools.partial(move_kernel, plan, batches),
        out_shape=jax.ShapeDtypeStruct((plan.nvir,) + send.shape, send.dtype),
        in_specs=[pl.BlockSpec(memory_space=pltpu.VMEM)],
        out_specs=pl.BlockSpec(memory_space=pl.ANY),
        scratch_shapes=[
            pltpu.SemaphoreType.DMA((3, plan.nvir, count)),
            pltpu.SemaphoreType.DMA((plan.nvir, count)),
            pltpu.SemaphoreType.DMA((count,)),
        ],
        compiler_params=pltpu.CompilerParams(collective_id=number, has_side_effects=True),
        name="move",
    )(send)


def gather_rows(plan, table, send):
    if not plan.aligned():
        full = lax.all_gather(send, "vir", axis=0)
        return full.transpose(1, 0, 2, 3).reshape(1, plan.units, LANES, plan.width)
    sizes = sorted({cdiv(plan.tiles * p, plan.groups) for p in range(4, plan.pairs + 1)} | {plan.units})
    branches = [
        functools.partial(lambda units, number, rows: move(plan, rows, units, 4, number), units, number)
        for number, units in enumerate(sizes)
    ]
    which = jnp.sum((jnp.array(sizes, jnp.int32) < table[plan.n_units]).astype(jnp.int32))
    return lax.switch(which, branches, send)


def energy_kernel(
    plan, acount, tb, table, occ, ints, gath, hole_amps, hole_ints, eab, ec, out, ibuf, gbuf, part, isem, gsem
):
    width = plan.width
    n_pairs = table[plan.n_pairs]
    n_units = table[plan.n_units]
    ow = plan.ow

    def slab(k):
        return pltpu.make_async_copy(ints.at[k], ibuf.at[k], isem.at[k])

    def rows(u):
        return pltpu.make_async_copy(gath.at[:, u], gbuf.at[u], gsem.at[u])

    out[...] = jnp.zeros_like(out)
    rows(0).start()
    for k in range(ow):
        slab(k).start()

    @pl.loop(1, n_units)
    def _(u):
        rows(u).start()

    for k in range(ow):
        slab(k).wait()

    @pl.loop(0, n_units)
    def _(u):
        rows(u).wait()
        p = table[plan.unit_pair + u]
        tile = table[plan.unit_tile + u]

        @pl.when(p < n_pairs)
        def _():
            key = table[plan.key + p]
            k = key // ow
            j = key % ow
            block = gbuf[u].reshape(LANES, width)
            for a in range(acount):
                part[a] = lax.dot_general(
                    ibuf[k, a], block, (((1,), (1,)), ((), ())), preferred_element_type=jnp.float32
                )
            holes = hole_ints[key, tile]
            ec_row = ec[tile]

            @pl.loop(table[plan.first + p], table[plan.first + p + 1])
            def _(pos):
                n = table[plan.order + pos]
                i = table[plan.occ_i + pos]
                shifted = ec_row - (occ[i] + occ[j] + occ[k])
                for a in range(acount):
                    acc = jnp.zeros((8, LANES), jnp.float32)
                    for t in range(width // tb):
                        at = pl.ds(t * tb, tb)
                        hole = jnp.dot(hole_amps[i, a, at], holes, preferred_element_type=jnp.float32)
                        amp = part[a, at] - hole
                        num = amp * amp
                        den = eab[a, at] + shifted
                        for _ in range(2):
                            half = num.shape[0] // 2
                            n0, n1 = num[:half], num[half:]
                            d0, d1 = den[:half], den[half:]
                            num = n0 * d1 + n1 * d0
                            den = d0 * d1
                        ratio = num / den
                        acc = acc + ratio.reshape(-1, 8, LANES).sum(axis=0)
                    out[n, a] = out[n, a] + acc


def energies(plan, table, occ, ints, gath, hole_amps, hole_ints, eab, ec):
    acount = ints.shape[1]
    smem = pl.BlockSpec(memory_space=pltpu.SMEM)
    vmem = pl.BlockSpec(memory_space=pltpu.VMEM)
    anys = pl.BlockSpec(memory_space=pl.ANY)
    front, units, back, width = gath.shape
    return pl.pallas_call(
        functools.partial(energy_kernel, plan, acount, 128),
        out_shape=jax.ShapeDtypeStruct((plan.total, acount, 8, LANES), jnp.float32),
        in_specs=[smem, smem, anys, anys, vmem, vmem, vmem, vmem],
        out_specs=vmem,
        scratch_shapes=[
            pltpu.VMEM(ints.shape, ints.dtype),
            pltpu.VMEM((units, front, back, width), gath.dtype),
            pltpu.VMEM((acount, width, LANES), jnp.float32),
            pltpu.SemaphoreType.DMA((plan.ow,)),
            pltpu.SemaphoreType.DMA((units,)),
        ],
        compiler_params=pltpu.CompilerParams(vmem_limit_bytes=VMEM_LIMIT),
        name="energy",
    )(table, occ, ints, gath, hole_amps, hole_ints, eab, ec)


def pick_energy(a_pick, vir_energy):
    columns = jnp.arange(vir_energy.shape[0], dtype=jnp.int32)
    return jnp.sum(jnp.where(a_pick[:, None] == columns[None, :], vir_energy[None, :], 0.0), axis=1)


def shards(
    triplets, counts, weights, a_pick, occ_energy, vir_energy, ints_vvvo, t2pair, t2hole, ints_hole
):
    slots = triplets.shape[0]
    groups = lax.axis_size("grp")
    nvir = lax.axis_size("vir")
    group_index = lax.axis_index("grp")
    a_count = a_pick.shape[0]
    window = a_count * nvir
    ow, holes = t2hole.shape[0], t2hole.shape[1]
    width = vir_energy.shape[0]
    plan = Plan(groups, nvir, slots, ow, width)

    mine = jnp.concatenate([counts, triplets.reshape(-1), weights])
    meta = lax.all_gather(mine, "grp", axis=0)
    table, send = make_plan(plan, meta, t2pair)
    gath = gather_rows(plan, table, send)

    lane = jnp.arange(width, dtype=jnp.int32)
    tile, v, r = lane // LANES, (lane % LANES) // plan.rows, lane % plan.rows
    column = v * (width // nvir) + tile * plan.rows + r
    onehot = (jnp.arange(width, dtype=jnp.int32)[:, None] == column[None, :]).astype(jnp.bfloat16)
    pad = (-holes) % 16
    hole_ints = jnp.pad(ints_hole, ((0, 0), (0, 0), (0, pad), (0, 0))).reshape(-1, width)
    hole_ints = jnp.dot(hole_ints, onehot, preferred_element_type=jnp.float32).astype(jnp.bfloat16)
    hole_ints = hole_ints.reshape(ow * ow, holes + pad, plan.tiles, LANES).transpose(0, 2, 1, 3)
    hole_amps = jnp.pad(t2hole, ((0, 0), (0, pad), (0, 0), (0, 0))).transpose(0, 2, 3, 1)
    ec = vir_energy.reshape(nvir, plan.tiles, plan.rows).transpose(1, 0, 2).reshape(plan.tiles, 1, LANES)
    a_energy = pick_energy(a_pick, vir_energy)
    eab = jnp.broadcast_to(
        (a_energy[:, None] + vir_energy[None, :])[:, :, None], (a_count, width, LANES)
    )

    raw = energies(plan, table, occ_energy, ints_vvvo, gath, hole_amps, hole_ints, eab, ec)
    factor = -meta[:, 1 + 3 * slots :].reshape(-1).astype(jnp.float32) / (width * width)
    energy = jnp.sum(raw, axis=(2, 3)) * factor[:, None]
    within = lax.psum(jnp.sum(energy, axis=1), "vir")
    trip_total, orbital_total = lax.psum((within, jnp.sum(energy, axis=0)), "grp")
    trip_energy = lax.dynamic_slice_in_dim(trip_total, group_index * slots, slots, 0) / window
    return (trip_energy, orbital_total)


def solution(mesh):
    placed = (
        P("grp", None),
        P("grp"),
        P("grp"),
        P("vir"),
        P(),
        P(),
        P(None, "vir", None, None),
        P(None, None, "vir", None),
        P(None, None, "vir", None),
        P(),
    )
    return jax.shard_map(
        shards, mesh=mesh, in_specs=placed, out_specs=(P("grp"), P("vir")), check_vma=False
    )
```

```python
import functools

import jax
import jax.numpy as jnp
from jax import lax
from jax.experimental import pallas as pl
from jax.experimental.pallas import tpu as pltpu
from jax.sharding import PartitionSpec as P

LANES = 128
BATCH = 2
LEAD = 2
VMEM_LIMIT = 60 * 1024 * 1024


def cdiv(a, b):
    return (a + b - 1) // b


class Plan:
    def __init__(self, groups, nvir, slots, ow, width):
        self.groups, self.nvir, self.slots, self.ow, self.width = groups, nvir, slots, ow, width
        self.total = groups * slots
        self.tiles = width // LANES
        self.rows = LANES // nvir
        self.pairs = min(ow * (ow + 1) // 2, self.total)
        self.units = cdiv(cdiv(self.tiles * self.pairs, groups), BATCH) * BATCH
        self.keys = ow * ow
        self.n_pairs = 0
        self.n_units = 1
        self.first = 2
        self.key = self.first + self.pairs + 1
        self.order = self.key + self.pairs + 1
        self.occ_i = self.order + self.total
        self.unit_pair = self.occ_i + self.total
        self.unit_tile = self.unit_pair + self.units
        self.unit_key = self.unit_tile + self.units
        self.unit_i = self.unit_key + self.units
        self.size = self.unit_i + self.units

    def aligned(self):
        return self.rows % 16 == 0 and self.nvir % 2 == 0


def plan_kernel(plan, with_rows, meta, *refs):
    if with_rows:
        t2pair, table, send, count, place, sems = refs
    else:
        table, count, place = refs
    group = lax.axis_index("grp")
    slots, ow = plan.slots, plan.ow

    def fields(n):
        g = n // slots
        s = n % slots
        live = s < meta[g, 0]
        at = 1 + 3 * s
        return live, meta[g, at], meta[g, at + 1], meta[g, at + 2]

    for key in range(plan.keys):
        count[key] = 0
    for n in range(plan.total):
        live, i, j, k = fields(n)
        key = k * ow + j
        count[key] = count[key] + live.astype(jnp.int32)
    pair = jnp.int32(0)
    pos = jnp.int32(0)
    table[plan.key] = 0
    for key in range(plan.keys):
        here = count[key]
        place[key] = pos

        @pl.when(here > 0)
        def _():
            table[plan.first + pair] = pos
            table[plan.key + pair] = key

        pair = pair + (here > 0).astype(jnp.int32)
        pos = pos + here
    table[plan.first + pair] = pos
    n_units = (plan.tiles * pair + plan.groups - 1) // plan.groups
    table[plan.n_pairs] = pair
    table[plan.n_units] = n_units
    for n in range(plan.total):
        live, i, j, k = fields(n)
        key = k * ow + j

        @pl.when(live)
        def _():
            at = place[key]
            table[plan.order + at] = n
            table[plan.occ_i + at] = i
            place[key] = at + 1

    for u in range(plan.units):
        q = u * plan.groups + group
        p = q // plan.tiles
        real = p < pair
        used = jnp.where(real, p, 0)
        key = table[plan.key + used]
        table[plan.unit_pair + u] = jnp.where(real, p, plan.pairs)
        table[plan.unit_tile + u] = q % plan.tiles
        table[plan.unit_key + u] = key
        table[plan.unit_i + u] = table[plan.occ_i + table[plan.first + used]]
        if with_rows:
            tile = pl.multiple_of((q % plan.tiles) * plan.rows, plan.rows)
            pltpu.make_async_copy(
                t2pair.at[key % ow, key // ow, pl.ds(tile, plan.rows), :], send.at[u], sems.at[u]
            ).start()
    if with_rows:
        for u in range(plan.units):
            pltpu.make_async_copy(t2pair.at[0, 0, pl.ds(0, plan.rows), :], send.at[u], sems.at[u]).wait()


def make_plan(plan, meta, t2pair):
    with_rows = plan.aligned()
    smem = pl.BlockSpec(memory_space=pltpu.SMEM)
    table_shape = jax.ShapeDtypeStruct((plan.size,), jnp.int32)
    scratch = [pltpu.SMEM((plan.keys,), jnp.int32), pltpu.SMEM((plan.keys,), jnp.int32)]
    if with_rows:
        send_shape = jax.ShapeDtypeStruct((plan.units, plan.rows, plan.width), t2pair.dtype)
        return pl.pallas_call(
            functools.partial(plan_kernel, plan, True),
            out_shape=(table_shape, send_shape),
            in_specs=[smem, pl.BlockSpec(memory_space=pl.ANY)],
            out_specs=(smem, pl.BlockSpec(memory_space=pltpu.VMEM)),
            scratch_shapes=scratch + [pltpu.SemaphoreType.DMA((plan.units,))],
            name="plan",
        )(meta, t2pair)
    table = pl.pallas_call(
        functools.partial(plan_kernel, plan, False),
        out_shape=table_shape,
        in_specs=[smem],
        out_specs=smem,
        scratch_shapes=scratch,
        name="plan",
    )(meta)
    key = lax.dynamic_slice_in_dim(table, plan.unit_key, plan.units)
    tile = lax.dynamic_slice_in_dim(table, plan.unit_tile, plan.units)
    cut = t2pair.reshape(plan.ow, plan.ow, plan.tiles, plan.rows, plan.width)
    return table, cut[key % plan.ow, key // plan.ow, tile]


def exchange_kernel(axes, ndev, nvir, src, out, ssem, rsem, lsem):
    me = lax.axis_index(axes[0])
    for axis in axes[1:]:
        me = me * lax.axis_size(axis) + lax.axis_index(axis)

    def device(to):
        return {"grp": to // nvir, "vir": to % nvir} if len(axes) == 2 else {axes[0]: to}

    barrier = pltpu.get_barrier_semaphore()

    @pl.loop(1, ndev)
    def _(d):
        pl.semaphore_signal(barrier, inc=1, device_id=device((me + d) % ndev))

    pl.semaphore_wait(barrier, ndev - 1)

    def copy(slot, to, d):
        return pltpu.make_async_remote_copy(
            src_ref=src,
            dst_ref=out.at[slot],
            send_sem=ssem.at[d],
            recv_sem=rsem.at[slot],
            device_id=device(to),
        )

    @pl.loop(1, ndev)
    def _(d):
        copy(me, (me + d) % ndev, d).start()

    own = pltpu.make_async_copy(src, out.at[me], lsem)
    own.start()
    own.wait()

    @pl.loop(1, ndev)
    def _(d):
        copy((me + ndev - d) % ndev, (me + d) % ndev, d).wait_recv()

    @pl.loop(1, ndev)
    def _(d):
        copy(me, (me + d) % ndev, d).wait_send()


def exchange(block, axes, sizes, number):
    ndev = 1
    for size in sizes:
        ndev *= size
    vmem = pl.BlockSpec(memory_space=pltpu.VMEM)
    return pl.pallas_call(
        functools.partial(exchange_kernel, axes, ndev, sizes[-1]),
        out_shape=jax.ShapeDtypeStruct((ndev,) + block.shape, block.dtype),
        in_specs=[vmem],
        out_specs=vmem,
        scratch_shapes=[
            pltpu.SemaphoreType.DMA((ndev,)),
            pltpu.SemaphoreType.DMA((ndev,)),
            pltpu.SemaphoreType.DMA,
        ],
        compiler_params=pltpu.CompilerParams(collective_id=number, has_side_effects=True),
        name="exchange",
    )(block)


def job(part, amps, holes, eab, shifted, i, a, width, tb):
    acc = jnp.zeros((8, LANES), jnp.float32)
    for t in range(width // tb):
        at = pl.ds(t * tb, tb)
        hole = jnp.dot(amps[i, a, at], holes, preferred_element_type=jnp.float32)
        amp = part[a, at] - hole
        num = amp * amp
        den = eab[a, at] + shifted
        for _ in range(2):
            half = num.shape[0] // 2
            n0, n1 = num[:half], num[half:]
            d0, d1 = den[:half], den[half:]
            num = n0 * d1 + n1 * d0
            den = d0 * d1
        ratio = num / den
        acc = acc + ratio.reshape(-1, 8, LANES).sum(axis=0)
    return acc


def work_kernel(plan, units, remote, table, occ, send, ints, hole_in, amps_in, eab, ec, first_out, parts, holes, amps, *scratch):
    gath, ibuf, hbuf, part, isem, psem, ssem, rsem, lsem = scratch
    if not remote:
        gath = send
    width, ow, acount = plan.width, plan.ow, ints.shape[1]
    count = units // BATCH
    nvir = plan.nvir
    chips = nvir // 2
    me = lax.axis_index("vir")
    z = me // 2
    core = me % 2
    partner = me + 1 - 2 * core
    right = jnp.minimum(z + 1, chips - 1) * 2 + core
    left = jnp.maximum(z - 1, 0) * 2 + core
    has_right = z < chips - 1
    has_left = z > 0

    def slab(k):
        return pltpu.make_async_copy(ints.at[k], ibuf.at[k], isem.at[k])

    for k in range(ow):
        slab(k).start()

    def copy(b, v, to, way, own=False):
        block = gath.at[v, pl.ds(b * BATCH, BATCH)]
        return pltpu.make_async_remote_copy(
            src_ref=send.at[pl.ds(b * BATCH, BATCH)] if own else block,
            dst_ref=block,
            send_sem=ssem.at[way, v, b],
            recv_sem=rsem.at[v, b],
            device_id={"vir": to},
        )

    def local(b):
        return pltpu.make_async_copy(
            send.at[pl.ds(b * BATCH, BATCH)], gath.at[me, pl.ds(b * BATCH, BATCH)], lsem.at[b]
        )

    def send_own(b):
        @pl.when(has_right)
        def _():
            copy(b, me, right, 0, True).start()

        @pl.when(has_left)
        def _():
            copy(b, me, left, 1, True).start()

        copy(b, me, partner, 2, True).start()
        local(b).start()

    def flows(d):
        return (
            (0, me - 2 * d, z - d >= 0, has_right, right),
            (1, me + 2 * d, z + d < chips, has_left, left),
        )

    if remote:
        barrier = pltpu.get_barrier_semaphore()
        pl.semaphore_signal(barrier, inc=1, device_id={"vir": partner})

        @pl.when(has_right)
        def _():
            pl.semaphore_signal(barrier, inc=1, device_id={"vir": right})

        @pl.when(has_left)
        def _():
            pl.semaphore_signal(barrier, inc=1, device_id={"vir": left})

        pl.semaphore_wait(barrier, 1 + has_right.astype(jnp.int32) + has_left.astype(jnp.int32))
        for b in range(min(LEAD, count)):
            send_own(b)

    def prepare():
        hbuf[...] = jnp.zeros_like(hbuf)
        for key in range(plan.keys):
            hbuf[key, : hole_in.shape[1]] = hole_in[key]
        flat = hbuf[...].reshape(-1, width)
        row = lax.broadcasted_iota(jnp.int32, (width, LANES), 0)
        lane = lax.broadcasted_iota(jnp.int32, (width, LANES), 1)
        column = (lane // plan.rows) * (width // nvir) + lane % plan.rows

        @pl.loop(0, plan.tiles)
        def _(tile):
            pick = (row == column + tile * plan.rows).astype(jnp.float32).astype(jnp.bfloat16)
            holes[tile] = (
                jnp.dot(flat, pick, preferred_element_type=jnp.float32)
                .astype(jnp.bfloat16)
                .reshape(plan.keys, -1, LANES)
            )

        for i in range(ow):
            for a in range(acount):
                amps[i, a] = amps_in[i, a].astype(jnp.float32).T.astype(jnp.bfloat16)

    def relay(s):
        for d in range(1, chips):
            b = s - (d - 1)
            inside = jnp.logical_and(b >= 0, b < count)
            for way, source, there, more, to in flows(d):

                @pl.when(jnp.logical_and(inside, there))
                def _():
                    copy(b, source, partner, 2).wait_recv()

                    @pl.when(more)
                    def _():
                        copy(b, source, to, way).start()

                    copy(b, source, partner, 2).start()

        @pl.when(s + LEAD < count)
        def _():
            send_own(s + LEAD)

    def stored(u):
        return pltpu.make_async_copy(part.at[u % 2], parts.at[u], psem.at[u % 2])

    def compute(b):
        if remote:
            local(b).wait()
            for other in range(chips):
                copy(b, 2 * other + 1 - core, partner, 2).wait_recv()

        @pl.loop(0, BATCH)
        def _(m):
            u = b * BATCH + m
            slot = u % 2

            @pl.when(u >= 2)
            def _():
                stored(u).wait()

            key = table[plan.unit_key + u]
            tile = table[plan.unit_tile + u]
            i = table[plan.unit_i + u]
            k = key // ow
            j = key % ow
            block = gath[:, u].reshape(LANES, width)
            hole = holes[tile, key]
            shifted = ec[tile] - (occ[i] + occ[j] + occ[k])
            for a in range(acount):
                part[slot, a] = lax.dot_general(
                    ibuf[k, a], block, (((1,), (1,)), ((), ())), preferred_element_type=jnp.float32
                )
                first_out[u, a] = job(part.at[slot], amps, hole, eab, shifted, i, a, width, LANES)
            stored(u).start()

    if remote:
        relay(jnp.int32(0))
    prepare()
    for k in range(ow):
        slab(k).wait()
    if remote:

        @pl.loop(1, count + chips - 1)
        def _(s):
            relay(s)

            @pl.when(s >= chips - 1)
            def _():
                compute(s - (chips - 1))

        @pl.loop(0, count)
        def _(b):
            @pl.when(has_right)
            def _():
                copy(b, me, right, 0, True).wait_send()

            @pl.when(has_left)
            def _():
                copy(b, me, left, 1, True).wait_send()

            copy(b, me, partner, 2, True).wait_send()
            for d in range(1, chips):
                for way, source, there, more, to in flows(d):

                    @pl.when(there)
                    def _():
                        @pl.when(more)
                        def _():
                            copy(b, source, to, way).wait_send()

                        copy(b, source, partner, 2).wait_send()
    else:

        @pl.loop(0, count)
        def _(b):
            compute(b)

    stored(0).wait()
    stored(1).wait()


def work(plan, units, remote, number, table, occ, send, ints, hole_in, amps_in, eab, ec):
    smem = pl.BlockSpec(memory_space=pltpu.SMEM)
    vmem = pl.BlockSpec(memory_space=pltpu.VMEM)
    anys = pl.BlockSpec(memory_space=pl.ANY)
    acount, width, depth = ints.shape[1], plan.width, amps_in.shape[2]
    count = units // BATCH
    chips = max(plan.nvir // 2, 1)
    held = (plan.nvir, units, plan.rows, width) if remote else (16, LANES)
    params = dict(vmem_limit_bytes=VMEM_LIMIT)
    if remote:
        params.update(collective_id=number, has_side_effects=True)
    return pl.pallas_call(
        functools.partial(work_kernel, plan, units, remote),
        out_shape=(
            jax.ShapeDtypeStruct((plan.units, acount, 8, LANES), jnp.float32),
            jax.ShapeDtypeStruct((plan.units, acount, width, LANES), jnp.float32),
            jax.ShapeDtypeStruct((plan.tiles, plan.keys, depth, LANES), jnp.bfloat16),
            jax.ShapeDtypeStruct((plan.ow, acount, width, depth), jnp.bfloat16),
        ),
        in_specs=[smem, smem, vmem, anys, vmem, vmem, vmem, vmem],
        out_specs=(vmem, anys, vmem, vmem),
        scratch_shapes=[
            pltpu.VMEM(held, ints.dtype),
            pltpu.VMEM(ints.shape, ints.dtype),
            pltpu.VMEM((plan.keys, depth, width), ints.dtype),
            pltpu.VMEM((2, acount, width, LANES), jnp.float32),
            pltpu.SemaphoreType.DMA((plan.ow,)),
            pltpu.SemaphoreType.DMA((2,)),
            pltpu.SemaphoreType.DMA((3, plan.nvir, count)),
            pltpu.SemaphoreType.DMA((plan.nvir, count)),
            pltpu.SemaphoreType.DMA((count,)),
        ],
        compiler_params=pltpu.CompilerParams(**params),
        name="work",
    )(table, occ, send, ints, hole_in, amps_in, eab, ec)


def first_work(plan, table, send, *operands):
    if not plan.aligned():
        full = lax.all_gather(send, "vir", axis=0)
        full = full.transpose(1, 0, 2, 3).reshape(1, plan.units, LANES, plan.width)
        return work(plan, plan.units, False, 0, table, operands[0], full, *operands[1:])
    sizes = set()
    for p in range(5, plan.pairs + 1):
        units = cdiv(cdiv(plan.tiles * p, plan.groups), BATCH) * BATCH
        sizes.add(units if p <= 12 else plan.units)
    sizes = sorted(sizes | {plan.units})
    branches = [
        functools.partial(lambda units, number, *ops: work(plan, units, True, number, *ops), units, 2 + at)
        for at, units in enumerate(sizes)
    ]
    which = jnp.sum((jnp.array(sizes, jnp.int32) < table[plan.n_units]).astype(jnp.int32))
    return lax.switch(which, branches, table, operands[0], send, *operands[1:])


def rest_kernel(plan, acount, table, occ, first_in, parts, holes, amps, eab, ec, out, pbuf, psem):
    width, ow = plan.width, plan.ow
    n_pairs = table[plan.n_pairs]
    n_units = table[plan.n_units]

    def fetch(u):
        return pltpu.make_async_copy(parts.at[u], pbuf.at[u], psem.at[u])

    def each(act):
        @pl.loop(0, n_units)
        def _(u):
            p = table[plan.unit_pair + u]

            @pl.when(p < n_pairs)
            def _():
                act(u, table[plan.first + p], table[plan.first + p + 1])

    def begin(u, lo, hi):
        @pl.when(hi - lo > 1)
        def _():
            fetch(u).start()

    def finish(u, lo, hi):
        n = table[plan.order + lo]
        out[n] = out[n] + first_in[u]

        @pl.when(hi - lo > 1)
        def _():
            fetch(u).wait()
            key = table[plan.unit_key + u]
            tile = table[plan.unit_tile + u]
            k = key // ow
            j = key % ow
            hole = holes[tile, key]

            @pl.loop(lo + 1, hi)
            def _(pos):
                n = table[plan.order + pos]
                i = table[plan.occ_i + pos]
                shifted = ec[tile] - (occ[i] + occ[j] + occ[k])
                for a in range(acount):
                    out[n, a] = out[n, a] + job(pbuf.at[u], amps, hole, eab, shifted, i, a, width, LANES)

    out[...] = jnp.zeros_like(out)
    each(begin)
    each(finish)


def rest(plan, table, occ, first_in, parts, holes, amps, eab, ec):
    acount = parts.shape[1]
    smem = pl.BlockSpec(memory_space=pltpu.SMEM)
    vmem = pl.BlockSpec(memory_space=pltpu.VMEM)
    anys = pl.BlockSpec(memory_space=pl.ANY)
    return pl.pallas_call(
        functools.partial(rest_kernel, plan, acount),
        out_shape=jax.ShapeDtypeStruct((plan.total, acount, 8, LANES), jnp.float32),
        in_specs=[smem, smem, vmem, anys, vmem, vmem, vmem, vmem],
        out_specs=vmem,
        scratch_shapes=[pltpu.VMEM(parts.shape, parts.dtype), pltpu.SemaphoreType.DMA((plan.units,))],
        compiler_params=pltpu.CompilerParams(vmem_limit_bytes=VMEM_LIMIT),
        name="rest",
    )(table, occ, first_in, parts, holes, amps, eab, ec)


def pick_energy(a_pick, vir_energy):
    columns = jnp.arange(vir_energy.shape[0], dtype=jnp.int32)
    return jnp.sum(jnp.where(a_pick[:, None] == columns[None, :], vir_energy[None, :], 0.0), axis=1)


def shards(
    triplets, counts, weights, a_pick, occ_energy, vir_energy, ints_vvvo, t2pair, t2hole, ints_hole
):
    slots = triplets.shape[0]
    groups = lax.axis_size("grp")
    nvir = lax.axis_size("vir")
    group_index = lax.axis_index("grp")
    a_count = a_pick.shape[0]
    window = a_count * nvir
    ow, holes = t2hole.shape[0], t2hole.shape[1]
    width = vir_energy.shape[0]
    plan = Plan(groups, nvir, slots, ow, width)

    mine = jnp.concatenate([counts, triplets.reshape(-1), weights])
    mine = jnp.pad(mine, (0, (-mine.shape[0]) % LANES)).reshape(-1, LANES)
    meta = exchange(mine, ("grp",), (groups,), 0).reshape(groups, -1)
    table, send = make_plan(plan, meta, t2pair)

    pad = (-holes) % 16
    hole_in = ints_hole.reshape(ow * ow, holes, width)
    amps_in = jnp.pad(t2hole.transpose(0, 2, 1, 3), ((0, 0), (0, 0), (0, pad), (0, 0)))
    ec = vir_energy.reshape(nvir, plan.tiles, plan.rows).transpose(1, 0, 2).reshape(plan.tiles, 1, LANES)
    a_energy = pick_energy(a_pick, vir_energy)
    eab = jnp.broadcast_to(
        (a_energy[:, None] + vir_energy[None, :])[:, :, None], (a_count, width, LANES)
    )

    first, parts, hole_ints, amps = first_work(
        plan, table, send, occ_energy, ints_vvvo, hole_in, amps_in, eab, ec
    )
    raw = rest(plan, table, occ_energy, first, parts, hole_ints, amps, eab, ec)
    factor = -meta[:, 1 + 3 * slots : 1 + 4 * slots].reshape(-1).astype(jnp.float32) / (width * width)
    energy = jnp.sum(raw, axis=(2, 3)) * factor[:, None]
    block = jnp.pad(energy.T, ((0, (-a_count) % 8), (0, (-plan.total) % LANES)))
    every = exchange(block, ("grp", "vir"), (groups, nvir), 1)
    trip_total = jnp.sum(every, axis=(0, 1))
    trip_energy = lax.dynamic_slice_in_dim(trip_total, group_index * slots, slots, 0) / window
    here = lax.dynamic_index_in_dim(
        every.reshape((groups, nvir) + block.shape), lax.axis_index("vir"), 1, keepdims=False
    )
    orbital_total = jnp.sum(here, axis=(0, 2))[:a_count]
    return (trip_energy, orbital_total)


def solution(mesh):
    placed = (
        P("grp", None),
        P("grp"),
        P("grp"),
        P("vir"),
        P(),
        P(),
        P(None, "vir", None, None),
        P(None, None, "vir", None),
        P(None, None, "vir", None),
        P(),
    )
    return jax.shard_map(
        shards, mesh=mesh, in_specs=placed, out_specs=(P("grp"), P("vir")), check_vma=False
    )
```

```python
import functools

import jax
import jax.numpy as jnp
from jax import lax
from jax.experimental import pallas as pl
from jax.experimental.pallas import tpu as pltpu
from jax.sharding import PartitionSpec as P

LANES = 128
BATCH = 2
LEAD = 4
VMEM_LIMIT = 60 * 1024 * 1024


def cdiv(a, b):
    return (a + b - 1) // b


class Plan:
    def __init__(self, groups, nvir, slots, ow, width):
        self.groups, self.nvir, self.slots, self.ow, self.width = groups, nvir, slots, ow, width
        self.total = groups * slots
        self.tiles = width // LANES
        self.rows = LANES // nvir
        self.pairs = min(ow * (ow + 1) // 2, self.total)
        self.units = cdiv(cdiv(self.tiles * self.pairs, groups), BATCH) * BATCH
        self.keys = ow * ow
        self.n_pairs = 0
        self.n_units = 1
        self.variant = 2
        self.first = 3
        self.key = self.first + self.pairs + 1
        self.order = self.key + self.pairs + 1
        self.occ_i = self.order + self.total
        self.unit_pair = self.occ_i + self.total
        self.unit_tile = self.unit_pair + self.units
        self.unit_key = self.unit_tile + self.units
        self.unit_i = self.unit_key + self.units
        self.size = self.unit_i + self.units

        sizes = {self.units}
        for p in range(5, min(self.pairs, 13)):
            sizes.add(cdiv(cdiv(self.tiles * p, groups), BATCH) * BATCH)
        self.sizes = sorted(sizes)

    def aligned(self):
        return self.rows % 16 == 0 and self.nvir % 2 == 0


def plan_kernel(plan, with_rows, meta, *refs):
    if with_rows:
        t2pair, table, send, count, place, sems = refs
    else:
        table, count, place = refs
    group = lax.axis_index("grp")
    slots, ow = plan.slots, plan.ow

    def fields(n):
        g = n // slots
        s = n % slots
        live = s < meta[g, 0]
        at = 1 + 3 * s
        return live, meta[g, at], meta[g, at + 1], meta[g, at + 2]

    for key in range(plan.keys):
        count[key] = 0
    for n in range(plan.total):
        live, i, j, k = fields(n)
        key = k * ow + j
        count[key] = count[key] + live.astype(jnp.int32)
    pair = jnp.int32(0)
    pos = jnp.int32(0)
    table[plan.key] = 0
    for key in range(plan.keys):
        here = count[key]
        place[key] = pos

        @pl.when(here > 0)
        def _():
            table[plan.first + pair] = pos
            table[plan.key + pair] = key

        pair = pair + (here > 0).astype(jnp.int32)
        pos = pos + here
    table[plan.first + pair] = pos
    n_units = (plan.tiles * pair + plan.groups - 1) // plan.groups
    table[plan.n_pairs] = pair
    table[plan.n_units] = n_units
    variant = jnp.int32(0)
    for units in plan.sizes[:-1]:
        variant = variant + (units < n_units).astype(jnp.int32)
    table[plan.variant] = variant
    for n in range(plan.total):
        live, i, j, k = fields(n)
        key = k * ow + j

        @pl.when(live)
        def _():
            at = place[key]
            table[plan.order + at] = n
            table[plan.occ_i + at] = i
            place[key] = at + 1

    for u in range(plan.units):
        q = u * plan.groups + group
        p = q // plan.tiles
        real = p < pair
        used = jnp.where(real, p, 0)
        key = table[plan.key + used]
        table[plan.unit_pair + u] = jnp.where(real, p, plan.pairs)
        table[plan.unit_tile + u] = q % plan.tiles
        table[plan.unit_key + u] = key
        table[plan.unit_i + u] = table[plan.occ_i + table[plan.first + used]]
        if with_rows:
            tile = pl.multiple_of((q % plan.tiles) * plan.rows, plan.rows)
            pltpu.make_async_copy(
                t2pair.at[key % ow, key // ow, pl.ds(tile, plan.rows), :], send.at[u], sems.at[u]
            ).start()
    if with_rows:
        for u in range(plan.units):
            pltpu.make_async_copy(t2pair.at[0, 0, pl.ds(0, plan.rows), :], send.at[u], sems.at[u]).wait()


def make_plan(plan, meta, t2pair):
    with_rows = plan.aligned()
    smem = pl.BlockSpec(memory_space=pltpu.SMEM)
    table_shape = jax.ShapeDtypeStruct((plan.size,), jnp.int32)
    scratch = [pltpu.SMEM((plan.keys,), jnp.int32), pltpu.SMEM((plan.keys,), jnp.int32)]
    if with_rows:
        send_shape = jax.ShapeDtypeStruct((plan.units, plan.rows, plan.width), t2pair.dtype)
        return pl.pallas_call(
            functools.partial(plan_kernel, plan, True),
            out_shape=(table_shape, send_shape),
            in_specs=[smem, pl.BlockSpec(memory_space=pl.ANY)],
            out_specs=(smem, pl.BlockSpec(memory_space=pltpu.VMEM)),
            scratch_shapes=scratch + [pltpu.SemaphoreType.DMA((plan.units,))],
            name="plan",
        )(meta, t2pair)
    table = pl.pallas_call(
        functools.partial(plan_kernel, plan, False),
        out_shape=table_shape,
        in_specs=[smem],
        out_specs=smem,
        scratch_shapes=scratch,
        name="plan",
    )(meta)
    key = lax.dynamic_slice_in_dim(table, plan.unit_key, plan.units)
    tile = lax.dynamic_slice_in_dim(table, plan.unit_tile, plan.units)
    cut = t2pair.reshape(plan.ow, plan.ow, plan.tiles, plan.rows, plan.width)
    return table, cut[key % plan.ow, key // plan.ow, tile]


def exchange_kernel(axes, ndev, nvir, src, out, ssem, rsem, lsem):
    me = lax.axis_index(axes[0])
    for axis in axes[1:]:
        me = me * lax.axis_size(axis) + lax.axis_index(axis)

    def device(to):
        return {"grp": to // nvir, "vir": to % nvir} if len(axes) == 2 else {axes[0]: to}

    barrier = pltpu.get_barrier_semaphore()

    @pl.loop(1, ndev)
    def _(d):
        pl.semaphore_signal(barrier, inc=1, device_id=device((me + d) % ndev))

    pl.semaphore_wait(barrier, ndev - 1)

    def copy(slot, to, d):
        return pltpu.make_async_remote_copy(
            src_ref=src,
            dst_ref=out.at[slot],
            send_sem=ssem.at[d],
            recv_sem=rsem.at[slot],
            device_id=device(to),
        )

    @pl.loop(1, ndev)
    def _(d):
        copy(me, (me + d) % ndev, d).start()

    own = pltpu.make_async_copy(src, out.at[me], lsem)
    own.start()
    own.wait()

    @pl.loop(1, ndev)
    def _(d):
        copy((me + ndev - d) % ndev, (me + d) % ndev, d).wait_recv()

    @pl.loop(1, ndev)
    def _(d):
        copy(me, (me + d) % ndev, d).wait_send()


def exchange(block, axes, sizes, number):
    ndev = 1
    for size in sizes:
        ndev *= size
    vmem = pl.BlockSpec(memory_space=pltpu.VMEM)
    return pl.pallas_call(
        functools.partial(exchange_kernel, axes, ndev, sizes[-1]),
        out_shape=jax.ShapeDtypeStruct((ndev,) + block.shape, block.dtype),
        in_specs=[vmem],
        out_specs=vmem,
        scratch_shapes=[
            pltpu.SemaphoreType.DMA((ndev,)),
            pltpu.SemaphoreType.DMA((ndev,)),
            pltpu.SemaphoreType.DMA,
        ],
        compiler_params=pltpu.CompilerParams(collective_id=number, has_side_effects=True),
        name="exchange",
    )(block)


def job(part, amps, holes, eab, shifted, i, a, width, tb):
    acc = jnp.zeros((8, LANES), jnp.float32)
    for t in range(width // tb):
        at = pl.ds(t * tb, tb)
        hole = jnp.dot(amps[i, a, at], holes, preferred_element_type=jnp.float32)
        amp = part[a, at] - hole
        num = amp * amp
        den = eab[a, at] + shifted
        for _ in range(2):
            half = num.shape[0] // 2
            n0, n1 = num[:half], num[half:]
            d0, d1 = den[:half], den[half:]
            num = n0 * d1 + n1 * d0
            den = d0 * d1
        ratio = num / den
        acc = acc + ratio.reshape(-1, 8, LANES).sum(axis=0)
    return acc


def work_kernel(plan, units, remote, table, occ, send, ints, hole_in, amps_in, eab, ec, first_out, parts, holes, amps, *scratch):
    gath, ibuf, hbuf, part, isem, psem, ssem, rsem, lsem = scratch
    if not remote:
        gath = send
    width, ow, acount = plan.width, plan.ow, ints.shape[1]
    count = units // BATCH
    nvir = plan.nvir
    chips = nvir // 2
    me = lax.axis_index("vir")
    z = me // 2
    core = me % 2
    partner = me + 1 - 2 * core
    right = jnp.minimum(z + 1, chips - 1) * 2 + core
    left = jnp.maximum(z - 1, 0) * 2 + core
    has_right = z < chips - 1
    has_left = z > 0

    def slab(k):
        return pltpu.make_async_copy(ints.at[k], ibuf.at[k], isem.at[k])

    for k in range(ow):
        slab(k).start()

    def copy(b, v, to, way, own=False):
        block = gath.at[v, pl.ds(b * BATCH, BATCH)]
        return pltpu.make_async_remote_copy(
            src_ref=send.at[pl.ds(b * BATCH, BATCH)] if own else block,
            dst_ref=block,
            send_sem=ssem.at[way, v, b],
            recv_sem=rsem.at[v, b],
            device_id={"vir": to},
        )

    def local(b):
        return pltpu.make_async_copy(
            send.at[pl.ds(b * BATCH, BATCH)], gath.at[me, pl.ds(b * BATCH, BATCH)], lsem.at[b]
        )

    def send_own(b):
        @pl.when(has_right)
        def _():
            copy(b, me, right, 0, True).start()

        @pl.when(has_left)
        def _():
            copy(b, me, left, 1, True).start()

        copy(b, me, partner, 2, True).start()
        local(b).start()

    def flows(d):
        return (
            (0, me - 2 * d, z - d >= 0, has_right, right),
            (1, me + 2 * d, z + d < chips, has_left, left),
        )

    if remote:
        barrier = pltpu.get_barrier_semaphore()
        pl.semaphore_signal(barrier, inc=1, device_id={"vir": partner})

        @pl.when(has_right)
        def _():
            pl.semaphore_signal(barrier, inc=1, device_id={"vir": right})

        @pl.when(has_left)
        def _():
            pl.semaphore_signal(barrier, inc=1, device_id={"vir": left})

        pl.semaphore_wait(barrier, 1 + has_right.astype(jnp.int32) + has_left.astype(jnp.int32))
        for b in range(min(LEAD, count)):
            send_own(b)

    def gather_holes():
        pad = hbuf.shape[1] - hole_in.shape[1]
        hbuf[:, hole_in.shape[1] :] = jnp.zeros((plan.keys, pad, width), hbuf.dtype)
        for key in range(plan.keys):
            hbuf[key, : hole_in.shape[1]] = hole_in[key]

    def pick_holes(first, last):
        flat = hbuf[...].reshape(-1, width)
        row = lax.broadcasted_iota(jnp.int32, (width, LANES), 0)
        lane = lax.broadcasted_iota(jnp.int32, (width, LANES), 1)
        column = (lane // plan.rows) * (width // nvir) + lane % plan.rows

        @pl.loop(first, last)
        def _(tile):
            pick = (row == column + tile * plan.rows).astype(jnp.float32).astype(jnp.bfloat16)
            holes[tile] = (
                jnp.dot(flat, pick, preferred_element_type=jnp.float32)
                .astype(jnp.bfloat16)
                .reshape(plan.keys, -1, LANES)
            )

    def turn_amps():
        @pl.loop(0, ow)
        def _(i):
            for a in range(acount):
                amps[i, a] = amps_in[i, a].astype(jnp.float32).T.astype(jnp.bfloat16)

    def relay(s):
        for d in range(1, chips):
            b = s - (d - 1)
            inside = jnp.logical_and(b >= 0, b < count)
            for way, source, there, more, to in flows(d):

                @pl.when(jnp.logical_and(inside, there))
                def _():
                    copy(b, source, partner, 2).wait_recv()

                    @pl.when(more)
                    def _():
                        copy(b, source, to, way).start()

                    copy(b, source, partner, 2).start()

        @pl.when(s + LEAD < count)
        def _():
            send_own(s + LEAD)

    def stored(u):
        return pltpu.make_async_copy(part.at[u % 2], parts.at[u], psem.at[u % 2])

    def compute(b):
        if remote:
            local(b).wait()
            for other in range(chips):
                copy(b, 2 * other + 1 - core, partner, 2).wait_recv()

        @pl.loop(0, BATCH)
        def _(m):
            u = b * BATCH + m
            slot = u % 2

            @pl.when(u >= 2)
            def _():
                stored(u).wait()

            key = table[plan.unit_key + u]
            tile = table[plan.unit_tile + u]
            i = table[plan.unit_i + u]
            k = key // ow
            j = key % ow
            block = gath[:, u].reshape(LANES, width)
            hole = holes[tile, key]
            shifted = ec[tile] - (occ[i] + occ[j] + occ[k])
            for a in range(acount):
                part[slot, a] = lax.dot_general(
                    ibuf[k, a], block, (((1,), (1,)), ((), ())), preferred_element_type=jnp.float32
                )
                first_out[u, a] = job(part.at[slot], amps, hole, eab, shifted, i, a, width, LANES)
            stored(u).start()

    turn_amps()
    gather_holes()
    fill = chips - 1 if remote else 1
    @pl.loop(0, count + fill)
    def _(s):
        if remote:
            relay(s)

        @pl.when(s < fill)
        def _():
            pick_holes(s * plan.tiles // fill, (s + 1) * plan.tiles // fill)

        @pl.when(s == fill)
        def _():
            for k in range(ow):
                slab(k).wait()

        @pl.when(s >= fill)
        def _():
            compute(s - fill)

    if remote:

        @pl.loop(0, count)
        def _(b):
            @pl.when(has_right)
            def _():
                copy(b, me, right, 0, True).wait_send()

            @pl.when(has_left)
            def _():
                copy(b, me, left, 1, True).wait_send()

            copy(b, me, partner, 2, True).wait_send()
            for d in range(1, chips):
                for way, source, there, more, to in flows(d):

                    @pl.when(there)
                    def _():
                        @pl.when(more)
                        def _():
                            copy(b, source, to, way).wait_send()

                        copy(b, source, partner, 2).wait_send()
    stored(0).wait()
    stored(1).wait()


def work(plan, units, remote, number, table, occ, send, ints, hole_in, amps_in, eab, ec):
    smem = pl.BlockSpec(memory_space=pltpu.SMEM)
    vmem = pl.BlockSpec(memory_space=pltpu.VMEM)
    anys = pl.BlockSpec(memory_space=pl.ANY)
    acount, width, depth = ints.shape[1], plan.width, amps_in.shape[2]
    count = units // BATCH
    chips = max(plan.nvir // 2, 1)
    held = (plan.nvir, units, plan.rows, width) if remote else (16, LANES)
    params = dict(vmem_limit_bytes=VMEM_LIMIT)
    if remote:
        params.update(collective_id=number, has_side_effects=True)
    return pl.pallas_call(
        functools.partial(work_kernel, plan, units, remote),
        out_shape=(
            jax.ShapeDtypeStruct((plan.units, acount, 8, LANES), jnp.float32),
            jax.ShapeDtypeStruct((plan.units, acount, width, LANES), jnp.float32),
            jax.ShapeDtypeStruct((plan.tiles, plan.keys, depth, LANES), jnp.bfloat16),
            jax.ShapeDtypeStruct((plan.ow, acount, width, depth), jnp.bfloat16),
        ),
        in_specs=[smem, smem, vmem, anys, vmem, vmem, vmem, vmem],
        out_specs=(vmem, anys, vmem, vmem),
        scratch_shapes=[
            pltpu.VMEM(held, ints.dtype),
            pltpu.VMEM(ints.shape, ints.dtype),
            pltpu.VMEM((plan.keys, depth, width), ints.dtype),
            pltpu.VMEM((2, acount, width, LANES), jnp.float32),
            pltpu.SemaphoreType.DMA((plan.ow,)),
            pltpu.SemaphoreType.DMA((2,)),
            pltpu.SemaphoreType.DMA((3, plan.nvir, count)),
            pltpu.SemaphoreType.DMA((plan.nvir, count)),
            pltpu.SemaphoreType.DMA((count,)),
        ],
        compiler_params=pltpu.CompilerParams(**params),
        name="work",
    )(table, occ, send, ints, hole_in, amps_in, eab, ec)


def first_work(plan, table, send, *operands):
    if not plan.aligned():
        full = lax.all_gather(send, "vir", axis=0)
        full = full.transpose(1, 0, 2, 3).reshape(1, plan.units, LANES, plan.width)
        return work(plan, plan.units, False, 0, table, operands[0], full, *operands[1:])
    branches = [
        functools.partial(lambda units, number, *ops: work(plan, units, True, number, *ops), units, 3 + at)
        for at, units in enumerate(plan.sizes)
    ]
    return lax.switch(table[plan.variant], branches, table, operands[0], send, *operands[1:])


def rest_kernel(plan, acount, table, occ, first_in, parts, holes, amps, eab, ec, out, pbuf, psem):
    width, ow = plan.width, plan.ow
    n_pairs = table[plan.n_pairs]
    n_units = table[plan.n_units]

    def fetch(u):
        return pltpu.make_async_copy(parts.at[u], pbuf.at[u], psem.at[u])

    def each(act):
        @pl.loop(0, n_units)
        def _(u):
            p = table[plan.unit_pair + u]

            @pl.when(p < n_pairs)
            def _():
                act(u, table[plan.first + p], table[plan.first + p + 1])

    def begin(u, lo, hi):
        @pl.when(hi - lo > 1)
        def _():
            fetch(u).start()

    def finish(u, lo, hi):
        n = table[plan.order + lo]
        out[n] = out[n] + first_in[u]

        @pl.when(hi - lo > 1)
        def _():
            fetch(u).wait()
            key = table[plan.unit_key + u]
            tile = table[plan.unit_tile + u]
            k = key // ow
            j = key % ow
            hole = holes[tile, key]

            @pl.loop(lo + 1, hi)
            def _(pos):
                n = table[plan.order + pos]
                i = table[plan.occ_i + pos]
                shifted = ec[tile] - (occ[i] + occ[j] + occ[k])
                for a in range(acount):
                    out[n, a] = out[n, a] + job(pbuf.at[u], amps, hole, eab, shifted, i, a, width, LANES)

    out[...] = jnp.zeros_like(out)
    each(begin)
    each(finish)


def rest(plan, table, occ, first_in, parts, holes, amps, eab, ec):
    acount = parts.shape[1]
    smem = pl.BlockSpec(memory_space=pltpu.SMEM)
    vmem = pl.BlockSpec(memory_space=pltpu.VMEM)
    anys = pl.BlockSpec(memory_space=pl.ANY)
    return pl.pallas_call(
        functools.partial(rest_kernel, plan, acount),
        out_shape=jax.ShapeDtypeStruct((plan.total, acount, 8, LANES), jnp.float32),
        in_specs=[smem, smem, vmem, anys, vmem, vmem, vmem, vmem],
        out_specs=vmem,
        scratch_shapes=[pltpu.VMEM(parts.shape, parts.dtype), pltpu.SemaphoreType.DMA((plan.units,))],
        compiler_params=pltpu.CompilerParams(vmem_limit_bytes=VMEM_LIMIT),
        name="rest",
    )(table, occ, first_in, parts, holes, amps, eab, ec)


def pick_energy(a_pick, vir_energy):
    columns = jnp.arange(vir_energy.shape[0], dtype=jnp.int32)
    return jnp.sum(jnp.where(a_pick[:, None] == columns[None, :], vir_energy[None, :], 0.0), axis=1)


def shards(
    triplets, counts, weights, a_pick, occ_energy, vir_energy, ints_vvvo, t2pair, t2hole, ints_hole
):
    slots = triplets.shape[0]
    groups = lax.axis_size("grp")
    nvir = lax.axis_size("vir")
    group_index = lax.axis_index("grp")
    a_count = a_pick.shape[0]
    window = a_count * nvir
    ow, holes = t2hole.shape[0], t2hole.shape[1]
    width = vir_energy.shape[0]
    plan = Plan(groups, nvir, slots, ow, width)

    mine = jnp.concatenate([counts, triplets.reshape(-1), weights])
    mine = jnp.pad(mine, (0, (-mine.shape[0]) % LANES)).reshape(-1, LANES)
    meta = exchange(mine, ("grp",), (groups,), 0).reshape(groups, -1)
    table, send = make_plan(plan, meta, t2pair)

    pad = (-holes) % 16
    hole_in = ints_hole.reshape(ow * ow, holes, width)
    amps_in = jnp.pad(t2hole.transpose(0, 2, 1, 3), ((0, 0), (0, 0), (0, pad), (0, 0)))
    ec = vir_energy.reshape(nvir, plan.tiles, plan.rows).transpose(1, 0, 2).reshape(plan.tiles, 1, LANES)
    a_energy = pick_energy(a_pick, vir_energy)
    eab = jnp.broadcast_to(
        (a_energy[:, None] + vir_energy[None, :])[:, :, None], (a_count, width, LANES)
    )

    first, parts, hole_ints, amps = first_work(
        plan, table, send, occ_energy, ints_vvvo, hole_in, amps_in, eab, ec
    )
    raw = rest(plan, table, occ_energy, first, parts, hole_ints, amps, eab, ec)
    factor = -meta[:, 1 + 3 * slots : 1 + 4 * slots].reshape(-1).astype(jnp.float32) / (width * width)
    energy = jnp.sum(raw, axis=(2, 3)) * factor[:, None]
    block = jnp.pad(energy.T, ((0, (-a_count) % 8), (0, (-plan.total) % LANES)))
    over_groups = jnp.sum(exchange(block, ("grp",), (groups,), 1), axis=0)
    orbital_total = jnp.sum(over_groups, axis=1)[:a_count]
    trip_total = jnp.sum(exchange(over_groups, ("vir",), (nvir,), 2), axis=(0, 1))
    trip_energy = lax.dynamic_slice_in_dim(trip_total, group_index * slots, slots, 0) / window
    return (trip_energy, orbital_total)


def solution(mesh):
    placed = (
        P("grp", None),
        P("grp"),
        P("grp"),
        P("vir"),
        P(),
        P(),
        P(None, "vir", None, None),
        P(None, None, "vir", None),
        P(None, None, "vir", None),
        P(),
    )
    return jax.shard_map(
        shards, mesh=mesh, in_specs=placed, out_specs=(P("grp"), P("vir")), check_vma=False
    )
```
